32 devices in a mesh: row: 8 (over z, core), col: 4 (over y, x).
Axes of the slice: x: 2, y: 2, z: 4, core: 2. Of those that a mesh axis runs over, the one named last changes fastest.
Arguments:
- hamiltonian: bfloat16 [36864, 36864], P('row', 'col'), may hold values from -0.6 to 0.6, as said below
- start_vectors: float32 [8, 4, 9216], P(None, 'col', 'row'), may hold values from -20 to 20
Outputs:
- last_vectors: float32 [8, 36864], P(None, ('row', 'col'))
- moments: float32 [8, 4], replicated
The draws below stay inside these ranges and needn't reach their ends.
Inputs may be any that keep to these rules, and one draw needn't show every extreme that they name: `hamiltonian`: the matrix is exactly symmetric.
All inputs are finite; a program needn't handle non-finite values.
Results may differ from the reference program's by a relative error of at most 0.0024.
Values may be sent and summed in bfloat16 or wider, within the bound.
No kernel may reach another device: no remote copies, remote signals or barrier semaphores. Data moves between devices by JAX's collectives and lax.ppermute only.
A program may use at most 128 MiB of HBM per device.

```python
import math
import jax
import jax.numpy as jnp
from jax import lax

NVEC = 8
STEPS = 3
ORDER = 36864
BLOCK_C = 9216


def draw_hamiltonian(key, part):
    tile_count = 16
    tile_width = ORDER // tile_count
    spread = 0.12 / math.sqrt(ORDER)
    offsets = jax.random.uniform(jax.random.fold_in(key, 7), (ORDER,), jnp.float32, -0.55, 0.55)
    base_key = jax.random.fold_in(key, 11)

    def random_tile(tile_number):
        tile_key = jax.random.fold_in(base_key, tile_number)
        values = jnp.clip(jax.random.normal(tile_key, (tile_width, tile_width), jnp.float32), -6.0, 6.0)
        return values * spread

    def row_strip(upper_index):

        def paired(other_index):
            return random_tile(upper_index * tile_count + other_index) + random_tile(other_index * tile_count + upper_index).T
        tiles = jax.vmap(paired)(jnp.arange(tile_count, dtype=jnp.int32))
        strip = jnp.moveaxis(tiles, 0, 1).reshape(tile_width, ORDER)
        diag_part = lax.dynamic_slice_in_dim(offsets, upper_index * tile_width, tile_width)
        rows_here = upper_index * tile_width + jnp.arange(tile_width, dtype=jnp.int32)
        on_diagonal = jnp.arange(ORDER, dtype=jnp.int32)[None, :] == rows_here[:, None]
        strip = strip + jnp.where(on_diagonal, diag_part[:, None], 0.0)
        return strip.astype(jnp.bfloat16)
    strips = lax.map(row_strip, jnp.arange(tile_count, dtype=jnp.int32))
    return strips.reshape(ORDER, ORDER)


def draw_start_vectors(key, part):
    ramp = jnp.arange(ORDER, dtype=jnp.float32) / ORDER
    scales = 10.0 ** (ramp - 0.5)
    values = scales[None, :] * jnp.clip(jax.random.normal(key, (NVEC, ORDER), jnp.float32), -6.0, 6.0)
    return values.reshape(NVEC, ORDER // BLOCK_C, BLOCK_C).astype(jnp.float32)


def setup_inputs(seed: int = 0) -> dict:
    seeds = jax.random.split(jax.random.key(seed), 3)
    return {
        "hamiltonian": draw_hamiltonian(jax.random.fold_in(seeds[2], 71), 0),
        "start_vectors": draw_start_vectors(jax.random.fold_in(seeds[2], 71), 0),
    }


def reference(hamiltonian, start_vectors):
    current = start_vectors.reshape(start_vectors.shape[0], -1)
    previous = current
    squares = [jnp.sum(current * current, axis=1) / ORDER]
    for level in range(STEPS):
        narrow = current.astype(jnp.bfloat16)
        applied = jnp.dot(narrow, hamiltonian, preferred_element_type=jnp.float32)
        if level == 0:
            following = applied
        else:
            following = 2.0 * applied - previous
        previous = current
        current = following
        squares.append(jnp.sum(current * current, axis=1) / ORDER)
    stacked = jnp.stack(squares, axis=1)
    moments = jnp.concatenate([stacked[:, :1], 2.0 * stacked[:, 1:] - stacked[:, :1]], axis=1)
    return current, moments
```

```python
import jax
import jax.numpy as jnp
from jax import lax
from jax.experimental import pallas as pl
from jax.experimental.pallas import tpu as pltpu
from jax.sharding import PartitionSpec as P

STEPS = 3
TILE = 256
VMEM_FOR_MATRIX = 60 * 1000 * 1000
SLOTS = 2


def vmem_spec():
    return pl.BlockSpec(memory_space=pltpu.VMEM)


def params(mib):
    return pltpu.CompilerParams(vmem_limit_bytes=mib * 1024 * 1024)


def start_kernel(v_ref, narrow_ref, sq_ref):
    v = v_ref[...]
    narrow_ref[...] = v.astype(jnp.bfloat16)
    lane = lax.broadcasted_iota(jnp.int32, sq_ref.shape, 1)
    sq_ref[...] = jnp.where(lane == 0, jnp.sum(v * v, axis=1, keepdims=True), 0.0)


def run_start(v):
    return pl.pallas_call(
        start_kernel,
        in_specs=[vmem_spec()],
        out_specs=[vmem_spec(), vmem_spec()],
        out_shape=[jax.ShapeDtypeStruct(v.shape, jnp.bfloat16), jax.ShapeDtypeStruct((v.shape[0], 128), jnp.float32)],
        compiler_params=params(2),
        name="start",
    )(v)


def column_block(width):
    for size in (1024, 768, 512, 256):
        if width % size == 0:
            return size
    return width


def kept_tiles(rows, width):
    tiles = rows // TILE
    block = column_block(width)
    best = 0
    for kept in range(1, tiles + 1):
        if TILE * 2 * (kept * width + SLOTS * (tiles - kept) * block) <= VMEM_FOR_MATRIX:
            best = kept
    return best


def run_apply(matrix, kept, narrow, count_parts, from_columns):
    first = kept is None
    rows, width = matrix.shape
    vec = narrow.shape[0]
    out_width = rows if from_columns else width
    w = out_width // count_parts
    block = column_block(width)
    count = width // block
    top = kept_tiles(rows, width) * TILE
    low = rows - top
    ahead = min(3, count)
    dims = (((1,), (1 if from_columns else 0,)), ((), ()))

    def apply_kernel(*refs):
        h_ref, v_ref = refs[:2]
        if first:
            kept_ref = refs[2]
        else:
            kept_ref, y_ref = refs[2:4]
        flat_ref, slots_ref, sems, kept_sems = refs[-4:]

        def columns(b):
            return pl.ds(pl.multiple_of(b * block, 128), block)

        def inside(b, n):
            return pl.ds(pl.multiple_of(b * block + n * TILE, 128), TILE)

        def keep(b):
            return pltpu.make_async_copy(
                h_ref.at[pl.ds(0, top), columns(b)], kept_ref.at[pl.ds(0, top), columns(b)], kept_sems.at[b])

        def fetch(b):
            slot = lax.rem(b, SLOTS)
            return pltpu.make_async_copy(h_ref.at[pl.ds(top, low), columns(b)], slots_ref.at[slot], sems.at[slot])

        def tile_product(v, tile):
            return lax.dot_general(v, tile, dims, preferred_element_type=jnp.float32)

        for b in range(max(SLOTS, ahead)):
            if first and b < ahead:
                keep(jnp.int32(b)).start()
            if b < SLOTS:
                fetch(jnp.int32(b)).start()
        if from_columns:
            flat_ref[...] = jnp.zeros_like(flat_ref)

        def body(b, carry):
            slot = lax.rem(b, SLOTS)
            if first:
                keep(b).wait()

            def tile_of(t, n):
                if t * TILE < top:
                    return kept_ref[t * TILE:(t + 1) * TILE, inside(b, n)]
                return slots_ref[slot, t * TILE - top:(t + 1) * TILE - top, n * TILE:(n + 1) * TILE]

            def rows_from(t0, t1):
                for t in range(t0, t1):
                    here = slice(t * TILE, (t + 1) * TILE)
                    if t * TILE < top:
                        tile = kept_ref[here, columns(b)]
                    else:
                        tile = slots_ref[slot, t * TILE - top:(t + 1) * TILE - top]
                    flat_ref[:, here] += tile_product(v_ref[:, columns(b)], tile)

            def columns_from(t0, t1, fresh):
                for n in range(block // TILE):
                    total = None if fresh else flat_ref[:, inside(b, n)]
                    for t in range(t0, t1):
                        part = tile_product(v_ref[:, t * TILE:(t + 1) * TILE], tile_of(t, n))
                        total = part if total is None else total + part
                    flat_ref[:, inside(b, n)] = total

            middle, end = top // TILE, rows // TILE
            if from_columns:
                rows_from(0, middle)
            else:
                columns_from(0, middle, True)
            fetch(b).wait()
            if from_columns:
                rows_from(middle, end)
            else:
                columns_from(middle, end, False)

            @pl.when(b + SLOTS < count)
            def _():
                fetch(b + SLOTS).start()

            if first:
                @pl.when(b + ahead < count)
                def _():
                    keep(b + ahead).start()
            return carry

        lax.fori_loop(0, count, body, 0)
        if first:
            left = flat_ref[...]
            terms = []
            for _ in range(3):
                term = left.astype(jnp.bfloat16).astype(jnp.float32)
                terms.append(term)
                left = left - term
            terms.append(jnp.zeros_like(left))
            kept_ref[top:top + 4 * vec, :out_width] = jnp.concatenate(terms, axis=0).astype(jnp.bfloat16)
        else:
            for g in range(count_parts):
                y_ref[g] = flat_ref[:, g * w:(g + 1) * w]

    y_shape = jax.ShapeDtypeStruct((count_parts, vec, w), jnp.float32)
    in_specs = [pl.BlockSpec(memory_space=pltpu.HBM), vmem_spec()]
    operands = [matrix, narrow]
    if first:
        out_shape = pltpu.VMEM((top + 4 * vec, width), jnp.bfloat16)
        out_specs = vmem_spec()
    else:
        out_shape = y_shape
        out_specs = vmem_spec()
        in_specs.append(vmem_spec())
        operands.append(pltpu.with_memory_space_constraint(kept, pltpu.VMEM))
    result = pl.pallas_call(
        apply_kernel,
        in_specs=in_specs,
        out_specs=out_specs,
        out_shape=out_shape,
        scratch_shapes=[
            pltpu.VMEM((vec, out_width), jnp.float32),
            pltpu.VMEM((SLOTS, low, block), jnp.bfloat16),
            pltpu.SemaphoreType.DMA((SLOTS,)),
            pltpu.SemaphoreType.DMA((count,)),
        ],
        compiler_params=params(10),
        name="first_apply" if first else "apply",
    )(*operands)
    return (run_extract(result, top, out_width, count_parts, vec), result) if first else (result, kept)


def run_extract(kept, top, out_width, count_parts, vec):
    w = out_width // count_parts

    def extract_kernel(kept_ref, y_ref):
        for g in range(count_parts):
            terms = kept_ref[top:top + 4 * vec, g * w:(g + 1) * w].astype(jnp.float32)
            y_ref[g] = (terms[:vec] + terms[vec:2 * vec]) + terms[2 * vec:3 * vec]

    return pl.pallas_call(
        extract_kernel,
        in_specs=[vmem_spec()],
        out_specs=vmem_spec(),
        out_shape=jax.ShapeDtypeStruct((count_parts, vec, w), jnp.float32),
        compiler_params=params(4),
        name="extract",
    )(pltpu.with_memory_space_constraint(kept, pltpu.VMEM))


def run_advance(parts, previous, sq, level):
    nr, vec, w = parts.shape

    def advance_kernel(parts_ref, prev_ref, sq_in_ref, v_ref, narrow_ref, sq_ref):
        v = jnp.sum(parts_ref[...], axis=0)
        if level > 0:
            v = 2.0 * v - prev_ref[...]
        v_ref[...] = v
        narrow_ref[...] = v.astype(jnp.bfloat16)
        lane = lax.broadcasted_iota(jnp.int32, sq_ref.shape, 1)
        sq_ref[...] = jnp.where(lane == level + 1, jnp.sum(v * v, axis=1, keepdims=True), sq_in_ref[...])

    return pl.pallas_call(
        advance_kernel,
        in_specs=[vmem_spec()] * 3,
        out_specs=[vmem_spec()] * 3,
        out_shape=[
            jax.ShapeDtypeStruct((vec, w), jnp.float32),
            jax.ShapeDtypeStruct((vec, w), jnp.bfloat16),
            jax.ShapeDtypeStruct(sq.shape, jnp.float32),
        ],
        compiler_params=params(2),
        name="advance",
    )(parts, previous, sq)


def finish(squares, order):
    squares = squares / order
    return jnp.concatenate([squares[:, :1], 2.0 * squares[:, 1:] - squares[:, :1]], axis=1)


def solution(mesh):
    nr = mesh.shape["row"]
    nc = mesh.shape["col"]

    def total(x):
        for axis, n in (("row", nr), ("col", nc)):
            d = 1
            while d < n:
                x = x + lax.ppermute(x, axis, [(i, i ^ d) for i in range(n)])
                d *= 2
        return x

    def kernels(hamiltonian, start_vectors):
        order = hamiltonian.shape[0] * nr
        v = start_vectors[:, 0, :]
        narrow, sq = run_start(v)
        kept = None
        previous = v
        for level in range(STEPS):
            from_columns = level % 2 == 0
            gather, scatter, n = ("row", "col", nc) if from_columns else ("col", "row", nr)
            gathered = lax.all_gather(narrow, gather, axis=1, tiled=True)
            parts, kept = run_apply(hamiltonian, kept, gathered, n, from_columns)
            parts = lax.all_to_all(parts, scatter, 0, 0, tiled=True)
            following, narrow, sq = run_advance(parts, previous, sq, level)
            previous, v = v, following
        moments = finish(total(sq)[:, :STEPS + 1], order)
        return v, moments

    def plain(hamiltonian, start_vectors):
        order = hamiltonian.shape[0] * nr
        current = start_vectors[:, 0, :]
        previous = current
        sums = [jnp.sum(current * current, axis=1)]
        for level in range(STEPS):
            narrow = current.astype(jnp.bfloat16)
            if level % 2 == 0:
                gathered = lax.all_gather(narrow, "row", axis=1, tiled=True)
                product = lax.dot_general(
                    gathered, hamiltonian, (((1,), (1,)), ((), ())), preferred_element_type=jnp.float32)
                axis, n = "col", nc
            else:
                gathered = lax.all_gather(narrow, "col", axis=1, tiled=True)
                product = jnp.dot(gathered, hamiltonian, preferred_element_type=jnp.float32)
                axis, n = "row", nr
            parts = product.reshape(product.shape[0], n, product.shape[1] // n)
            applied = lax.all_to_all(parts, axis, 1, 1, tiled=True).sum(axis=1)
            following = applied if level == 0 else 2.0 * applied - previous
            previous, current = current, following
            sums.append(jnp.sum(current * current, axis=1))
        return current, finish(total(jnp.stack(sums, axis=1)), order)

    def per_device(hamiltonian, start_vectors):
        rows, width = hamiltonian.shape
        aligned = rows % TILE == 0 and width % TILE == 0 and start_vectors.shape[2] % 128 == 0
        aligned = aligned and 0 < kept_tiles(rows, width) < rows // TILE
        if aligned:
            return kernels(hamiltonian, start_vectors)
        return plain(hamiltonian, start_vectors)

    return jax.shard_map(
        per_device,
        mesh=mesh,
        in_specs=(P("row", "col"), P(None, "col", "row")),
        out_specs=(P(None, ("row", "col")), P()),
        check_vma=False,
    )
```
